256 devices in a mesh: lat: 8 (over y, core), lon: 32 (over x, z).
Axes of the slice: x: 4, y: 4, z: 8, core: 2. Of those that a mesh axis runs over, the one named last changes fastest.
Arguments:
- ensemble: bfloat16 [8, 4, 32, 1536, 128], P(None, None, 'lat', 'lon'), may hold values from -5 to 5
- vert_loc: float32 [128, 128], replicated, may hold values from -0.5 to 0.5
- static_vert: float32 [128, 128], replicated, may hold values from -0.5 to 0.5
- inst_vert: float32 [16, 128], replicated, may hold values from -0.5 to 0.5
- inst_err: float32 [16], replicated, may hold values from 0.5 to 2
- obs_dest: int32 [65536, 1], P(('lat', 'lon')), may hold values from 0 to 255; in each aligned block of 256 rows (0 to 255, 256 to 511, ...) at most 2 rows name the same one
- obs_patch: int32 [65536], P(('lat', 'lon')), may hold values from 0 to 47
- obs_window: int32 [65536], P(('lat', 'lon')), may hold values from 0 to 3
- obs_inst: int32 [65536], P(('lat', 'lon')), may hold values from 0 to 15
- obs_hweight: float32 [4, 65536], P(None, ('lat', 'lon')), may hold values from 0 to 0.5
- innovation: float32 [65536], P(('lat', 'lon')), may hold values from -6 to 6
- obs_count: int32 [256], P(('lat', 'lon')), may hold values from 128 to 256, as said below
Outputs:
- static_control: float32 [32, 1536, 128], P('lat', 'lon')
- member_control: float32 [8, 32, 1536, 128], P(None, 'lat', 'lon')
- obs_equivalent: float32 [65536], P(('lat', 'lon'))
The draws below stay inside these ranges and needn't reach their ends.
Inputs may be any that keep to these rules, and one draw needn't show every extreme that they name: `obs_dest`: index of the tile in lat+lon order (lat slowest) that holds the row's patch; within the rows of one shard no tile is named more than 2 times. `obs_patch`: patch p of a tile covers its latitude rows 2 (p // 24) and the next, and its longitude columns 2 (p % 24) and the next. `obs_count`: some shard uses all 256 rows in every draw; rows at or past a shard's count are unused.
All inputs are finite; a program needn't handle non-finite values.
Results may differ from the reference program's by a relative error of at most 0.0003.
Values sent between devices are 32-bit elements; how exact they have to be, the bound alone decides.
A program may use at most 64 MiB of HBM per device.

```python
import math
import jax
import jax.numpy as jnp
import numpy as np
from jax import lax

CLAT = 4
CLON = 48
OBS_DEV = 256
MEM = 8
WIN = 4
NINST = 16
ITERS = 2
VL = 128
OWNERS = 256
NLAT = 32
NLON = 1536
NOBS = 65536
CAP = 2
PATCH_DEV = 48
N_LON = 32


def draw_obs_count(key, part):
    counts = jax.random.randint(key, (OWNERS,), OBS_DEV // 2, OBS_DEV + 1)
    fullest = jax.random.randint(jax.random.fold_in(key, 7), (), 0, OWNERS)
    return counts.at[fullest].set(OBS_DEV).astype(jnp.int32)


def with_ends(values, own_key, low, high):
    dims = values.shape
    place = [jax.random.randint(jax.random.fold_in(own_key, axis), (), 0, dims[axis]) for axis in range(len(dims))]
    values = values.at[tuple(place)].set(low)
    longest = dims.index(max(dims))
    place[longest] = (place[longest] + 1) % dims[longest]
    return values.at[tuple(place)].set(high)


def block_levels(rng, extent, split, low, largest):
    def one(dim, blocks):
        heights = jax.random.uniform(jax.random.fold_in(jax.random.fold_in(rng, 6), dim), (blocks,), jnp.float32, low / len(split), largest / len(split))
        return jnp.repeat(jnp.exp(heights), extent[dim] // blocks).reshape((-1,) + (1,) * (len(extent) - dim - 1))

    factor_of = one(*split[0])
    for cut in split[1:]:
        factor_of = factor_of * one(*cut)
    return factor_of


def deal_out(key, own, number, rows, amount, top, bound, skew):
    ranking = jax.random.permutation(key, amount)
    crowded, usual = shares(amount, rows * top, bound, skew, True), shares(amount, rows * top, bound, skew, False)
    places = jnp.arange(amount)

    def named(lengths, turn):
        used = int((lengths > 0).sum())
        fixed = max(1, used // 4)
        shifted = fixed + (places - fixed + turn * (used - fixed)) % max(1, amount - fixed)
        return jnp.zeros((amount,), jnp.int32).at[ranking[jnp.where(places < fixed, places, shifted)]].set(jnp.asarray(lengths, jnp.int32))

    lengths = jnp.where(number % 4 == 0, named(crowded, number // 4), named(usual, number - number // 4 - 1))
    mixed = jax.random.permutation(jax.random.fold_in(own, 3), amount)
    giver, receiver = mixed[0:amount // 2 * 2:2], mixed[1:amount // 2 * 2:2]
    margin = jnp.minimum(lengths[giver] - 1, bound - lengths[receiver]) // 2
    margin = jnp.where((giver == ranking[0]) | (receiver == ranking[0]) | (lengths[receiver] == 0), 0, jnp.maximum(margin, 0))
    shifted = jax.random.randint(jax.random.fold_in(own, 4), (amount // 2,), 0, 1 << 20) % (margin + 1)
    lengths = lengths.at[giver].add(-shifted).at[receiver].add(shifted)
    labels = jnp.searchsorted(jnp.cumsum(lengths), jnp.arange(rows * top), side="right").astype(jnp.int32)
    table = labels.reshape(top, rows).T
    table = table[jax.random.permutation(jax.random.fold_in(own, 1), rows)]
    turn = jax.random.randint(jax.random.fold_in(own, 2), (rows, 1), 0, top)
    return jnp.take_along_axis(table, (jnp.arange(top)[None, :] + turn) % top, axis=1)


def shares(number_of, total, reach, slope, full):
    portions = [(1 << 20) // math.isqrt(standing ** slope) + 1 for standing in range(1, number_of + 1)]
    largest = reach if full else min(reach, max(-(-total // number_of), total * portions[0] // sum(portions)))
    least = 1 if total - largest >= number_of - 1 else 0
    given, surplus = [largest] + [least] * (number_of - 1), total - largest - least * (number_of - 1)
    while surplus > 0:
        free = [i for i in range(1, number_of) if given[i] < largest] or [i for i in range(1, number_of) if given[i] < reach]
        mass, left = sum([portions[i] for i in free]), surplus
        for i in free:
            more = min(reach - given[i], max(1, left * portions[i] // mass), surplus)
            given[i] = given[i] + more
            surplus = surplus - more
    return np.array(given)


def bell_draw(own_key, shape, scale, reach, split=(), kind=jnp.bfloat16):
    values = jax.random.normal(own_key, shape, jnp.float32) * scale
    if len(split) > 0:
        values = block_levels(own_key, shape, split, -0.22, 0.18) * values
    return jnp.clip(values, min=-reach, max=reach).astype(kind)


def setup_inputs(seed: int = 0) -> dict:
    streams_of = jax.random.split(jax.random.key(seed), 13)
    ensemble = bell_draw(streams_of[0], (MEM, WIN, NLAT, NLON, VL), 0.35, 5.0, ((2, 8), (3, 32)))
    vert_loc = bell_draw(streams_of[1], (VL, VL), VL ** -0.5, 0.5, (), jnp.float32)
    static_vert = bell_draw(streams_of[2], (VL, VL), VL ** -0.5, 0.5, (), jnp.float32)
    inst_vert = bell_draw(streams_of[3], (NINST, VL), VL ** -0.5, 0.5, (), jnp.float32)
    inst_err = jnp.clip(jnp.exp(jax.random.uniform(streams_of[4], (NINST,), jnp.float32, math.log(0.5), math.log(2.0))), 0.5, 2.0)
    obs_dest_keys = jax.random.split(jax.random.fold_in(streams_of[5], 1), NOBS // OBS_DEV)
    obs_dest_turns = jax.random.permutation(jax.random.fold_in(streams_of[5], 3), NOBS // OBS_DEV)
    obs_dest = jax.vmap(lambda own, number: deal_out(jax.random.fold_in(streams_of[5], 2), own, number, OBS_DEV, OWNERS, 1, CAP, 2))(obs_dest_keys, obs_dest_turns).reshape((NOBS, 1))
    obs_patch = with_ends(jax.random.randint(streams_of[6], (NOBS,), 0, PATCH_DEV), jax.random.fold_in(streams_of[6], 1), 0, PATCH_DEV - 1).astype(jnp.int32)
    obs_window = with_ends(jax.random.randint(streams_of[7], (NOBS,), 0, WIN), jax.random.fold_in(streams_of[7], 1), 0, WIN - 1).astype(jnp.int32)
    obs_inst = with_ends(jax.random.randint(streams_of[8], (NOBS,), 0, NINST), jax.random.fold_in(streams_of[8], 1), 0, NINST - 1).astype(jnp.int32)
    obs_hweight = jnp.clip(0.5 * jax.random.uniform(streams_of[9], (4, NOBS), jnp.float32) ** block_levels(streams_of[9], (4, NOBS), ((1, 256),), -0.2, 0.2), 0.0, 0.5)
    innovation = bell_draw(streams_of[10], (NOBS,), 1.0, 6.0, ((0, 256),), jnp.float32)
    obs_count = draw_obs_count(jax.random.fold_in(streams_of[12], 71), 0)
    return {"ensemble": ensemble, "vert_loc": vert_loc, "static_vert": static_vert, "inst_vert": inst_vert, "inst_err": inst_err, "obs_dest": obs_dest, "obs_patch": obs_patch, "obs_window": obs_window, "obs_inst": obs_inst, "obs_hweight": obs_hweight, "innovation": innovation, "obs_count": obs_count}


SMOOTH = 0.15
BETA_STATIC = 0.5
BETA_ENSEMBLE = 0.85


def level_product(values, matrix):
    flat = values.reshape(-1, values.shape[-1])
    result = jnp.dot(flat, matrix, precision=lax.Precision.HIGHEST, preferred_element_type=jnp.float32)
    return result.reshape(values.shape[:-1] + (matrix.shape[1],))


def smooth_once(grid_field):
    widths = [(0, 0)] * (grid_field.ndim - 3) + [(1, 1), (0, 0), (0, 0)]
    padded = jnp.pad(grid_field, widths)
    northern = padded[..., :-2, :, :]
    southern = padded[..., 2:, :, :]
    eastern = jnp.roll(grid_field, -1, axis=grid_field.ndim - 2)
    western = jnp.roll(grid_field, 1, axis=grid_field.ndim - 2)
    return (1.0 - 4.0 * SMOOTH) * grid_field + SMOOTH * (northern + southern + eastern + western)


def spread(grid_field):
    return smooth_once(smooth_once(grid_field))


def combine(former, scale, latter):
    return (former[0] + scale * latter[0], former[1] + scale * latter[1])


def local_dot(former, latter):
    return jnp.sum(former[0] * latter[0]) + jnp.sum(former[1] * latter[1])


def reference(ensemble, vert_loc, static_vert, inst_vert, inst_err, obs_dest, obs_patch, obs_window, obs_inst, obs_hweight, innovation, obs_count):
    destination = obs_dest[:, 0]
    lat_start = (destination // N_LON) * CLAT + 2 * (obs_patch // (CLON // 2))
    lon_start = (destination % N_LON) * CLON + 2 * (obs_patch % (CLON // 2))
    row_index = jnp.arange(innovation.shape[0], dtype=jnp.int32)
    active = ((row_index % OBS_DEV) < obs_count[row_index // OBS_DEV]).astype(jnp.float32)
    hweights = obs_hweight * active[None, :]
    inverse_var = 1.0 / (inst_err[obs_inst] * inst_err[obs_inst])

    def forward(control):
        static_part = BETA_STATIC * level_product(spread(control[0]), static_vert)

        def add_member(summed, member_pair):
            member_weights, perturbation = member_pair
            localized = level_product(spread(member_weights), vert_loc)
            return summed + perturbation.astype(jnp.float32) * localized[None], None

        initial = jnp.zeros(ensemble.shape[1:], jnp.float32)
        summed, unused = lax.scan(add_member, initial, (control[1], ensemble))
        return static_part[None] + BETA_ENSEMBLE * summed

    def observe(increment):
        projected = level_product(increment, inst_vert.T)
        image = jnp.zeros(innovation.shape, jnp.float32)
        for corner in range(4):
            image = image + hweights[corner] * projected[obs_window, lat_start + corner // 2, lon_start + corner % 2, obs_inst]
        return image

    def gradient(weights):
        table = jnp.zeros(ensemble.shape[1:4] + (inst_vert.shape[0],), jnp.float32)
        for corner in range(4):
            table = table.at[obs_window, lat_start + corner // 2, lon_start + corner % 2, obs_inst].add(hweights[corner] * weights)
        return level_product(table, inst_vert)

    def adjoint(grad_field):
        static_part = BETA_STATIC * spread(level_product(jnp.sum(grad_field, axis=0), static_vert.T))

        def one_member(unused, perturbation):
            localized = jnp.sum(perturbation.astype(jnp.float32) * grad_field, axis=0)
            return unused, BETA_ENSEMBLE * spread(level_product(localized, vert_loc.T))

        unused, member_part = lax.scan(one_member, jnp.zeros((), jnp.float32), ensemble)
        return static_part, member_part

    def hessian(direction):
        obs_image = observe(forward(direction))
        back_field = adjoint(gradient(inverse_var * obs_image))
        return obs_image, combine(direction, 1.0, back_field)

    residual = adjoint(gradient(inverse_var * innovation))
    solution = (jnp.zeros_like(residual[0]), jnp.zeros_like(residual[1]))
    equivalent = jnp.zeros(innovation.shape, jnp.float32)
    direction = residual
    norm_now = local_dot(residual, residual)
    for iteration in range(ITERS):
        obs_image, image = hessian(direction)
        step_size = norm_now / local_dot(direction, image)
        solution = combine(solution, step_size, direction)
        equivalent = equivalent + step_size * obs_image
        residual = combine(residual, -step_size, image)
        norm_next = local_dot(residual, residual)
        direction = combine(residual, norm_next / norm_now, direction)
        norm_now = norm_next
    return solution[0], solution[1], equivalent
```

```python
import jax
import jax.numpy as jnp
from jax import lax
from jax.experimental import pallas as pl
from jax.experimental.pallas import tpu as pltpu
from jax.sharding import PartitionSpec as P

F32 = jnp.float32
HI = lax.Precision.HIGHEST
MESH = pl.DeviceIdType.MESH
SMOOTH = 0.15
BETA_STATIC = 0.5
BETA_ENSEMBLE = 0.85
NLAT, NLON = 8, 32
MEM, WIN, ROWS, COLS, LEV, NINST = 8, 4, 4, 48, 128, 16
FIELDS = MEM + 1
CELLS = ROWS * COLS
OBS = 256
PAD = 8
WIDE = COLS + 2 * PAD
TALL = 3 * ROWS
OWN = pl.ds(PAD, COLS)


def dot(a, b, precision=HI):
    return lax.dot_general(
        a, b, (((1,), (0,)), ((), ())), precision=precision, preferred_element_type=F32
    )


def dot_t(a, b, precision=HI):
    return lax.dot_general(
        a, b, (((1,), (1,)), ((), ())), precision=precision, preferred_element_type=F32
    )


def iota(shape, dim):
    return lax.broadcasted_iota(jnp.int32, shape, dim)


def total(x):
    return jnp.sum(jnp.sum(x, axis=1, keepdims=True), axis=0, keepdims=True)


def kernel(
    ens_hbm, vert_ref, static_ref, inst_ref, err_ref, dest_col_ref, dest_row_ref,
    patch_ref, window_ref, instr_ref, hweight_ref, innov_ref, count_ref,
    out_static, out_member, out_equiv,
    ens, send1, first1, flat1, second1, send2, first2, flat2, second2,
    red_a_send, red_a, red_b_send, red_b,
    place, onehot, onehot_t, spread_w, rinv, obs_e, obs_z, grad, incr,
    reg, strip_send, strip_recv, stage_a, stage_b, resid, acc,
    ens_sem, x1s, x1r, y1s, y1r, x2s, x2r, y2s, y2r, ras, rar, rbs, rbr, hs, hr,
):
    lat = lax.axis_index("lat")
    lon = lax.axis_index("lon")
    has_n = lat > 0
    has_s = lat < NLAT - 1
    west = lax.rem(lon + NLON - 1, NLON)
    east = lax.rem(lon + 1, NLON)
    base = lat * 16

    ens_copy = pltpu.make_async_copy(ens_hbm, ens, ens_sem)
    ens_copy.start()

    barrier = pltpu.get_barrier_semaphore()

    def greet(i, j):
        pl.semaphore_signal(barrier, inc=1, device_id=(i, j), device_id_type=MESH)

    def greet_lon(d, c):
        greet(lat, lax.rem(lon + d, NLON))
        return c

    def greet_lat(d, c):
        greet(lax.rem(lat + d, NLAT), lon)
        return c

    lax.fori_loop(1, NLON, greet_lon, 0)
    lax.fori_loop(1, NLAT, greet_lat, 0)

    for step in (1, NLAT - 1):
        greet(lax.rem(lat + step, NLAT), west)
        greet(lax.rem(lat + step, NLAT), east)

    dest_row = dest_row_ref[...]
    same = (dest_col_ref[...] == dest_row) & (iota((OBS, OBS), 0) < iota((OBS, OBS), 1))
    rank = jnp.sum(same.astype(F32), axis=0, keepdims=True)
    group = (dest_row >> 5) * 2 + rank.astype(jnp.int32)
    active = (iota((1, OBS), 1) < count_ref[...]).astype(F32)
    words = jnp.concatenate(
        [
            patch_ref[...].astype(F32),
            window_ref[...].astype(F32),
            instr_ref[...].astype(F32),
            hweight_ref[...] * active,
            innov_ref[...],
        ],
        axis=0,
    )
    tiled = jnp.concatenate([words] * 16, axis=0)
    tiled = jnp.where((iota((128, OBS), 0) >> 3) == group, tiled, 0.0)
    to_lon = (iota((NLON, OBS), 0) == (dest_row & 31)).astype(F32)
    outgoing = dot_t(to_lon, tiled)
    for j in range(NLON):
        send1[j] = outgoing[j : j + 1, :]

    place[...] = jnp.zeros_like(place)
    for c in range(4):
        place[c, 16 * c : 16 * c + 16, :] = inst_ref[...]
    for a in range(2):
        reg[a, :, :, 0:PAD, :] = jnp.zeros((FIELDS, TALL, PAD, LEV), F32)
        reg[a, :, :, PAD + COLS : WIDE, :] = jnp.zeros((FIELDS, TALL, PAD, LEV), F32)
    acc[...] = jnp.zeros_like(acc)

    pl.semaphore_wait(barrier, NLON - 1 + NLAT - 1 + 4)

    def remote(src, dst, ssem, rsem, i, j):
        return pltpu.make_async_remote_copy(
            src_ref=src, dst_ref=dst, send_sem=ssem, recv_sem=rsem,
            device_id=(i, j), device_id_type=MESH,
        )

    def rows_to_lon(send, first, ssem, rsem, one_row):
        def go(d, c):
            j = lax.rem(lon + d, NLON)
            src = send if one_row else send.at[j]
            remote(src, first.at[lon], ssem.at[j], rsem.at[lon], lat, j).start()
            return c

        lax.fori_loop(1, NLON, go, 0)
        first[lon] = send[...] if one_row else send[lon]

    def end_lon(send, first, ssem, rsem, one_row):
        def done(d, c):
            j = lax.rem(lon + d, NLON)
            src = send if one_row else send.at[j]
            remote(src, first.at[j], ssem.at[j], rsem.at[j], lat, j).wait()
            return c

        lax.fori_loop(1, NLON, done, 0)

    def block_to_lat(send, second, ssem, rsem):
        def go(d, c):
            i = lax.rem(lat + d, NLAT)
            remote(send, second.at[lat], ssem.at[i], rsem.at[lat], i, lon).start()
            return c

        lax.fori_loop(1, NLAT, go, 0)
        second[lat] = send[...]

    def end_lat(send, second, ssem, rsem):
        def done(d, c):
            i = lax.rem(lat + d, NLAT)
            remote(send, second.at[i], ssem.at[i], rsem.at[i], i, lon).wait()
            return c

        lax.fori_loop(1, NLAT, done, 0)

    def exchange(send, first, flat, second, xs, xr, ys, yr):
        rows_to_lon(send, first, xs, xr, False)
        end_lon(send, first, xs, xr, False)
        for j in range(NLON):
            flat[j : j + 1, :] = first[j]
        block_to_lat(flat, second, ys, yr)
        end_lat(flat, second, ys, yr)
        return second[...].reshape(NLAT * NLON, 128)

    received = exchange(send1, first1, flat1, second1, x1s, x1r, y1s, y1r)

    lane = iota((OBS, 128), 1)
    inst_lane = (lane & 15).astype(F32)
    err_row = err_ref[...]
    rinv_row = 1.0 / (err_row * err_row)
    row_w = iota((128, 128), 0)
    col_w = iota((128, 128), 1)
    for s in range(2):
        at = base + 8 * s
        l0 = iota((128, OBS), 0)
        pick = jnp.where(l0 == at, 1.0, 0.0) + jnp.where(l0 == at + 1, 48.0, 0.0)
        l1 = iota((OBS, 128), 1)
        pick_t = jnp.where(l1 == at, 1.0, 0.0) + jnp.where(l1 == at + 1, 48.0, 0.0)
        onehot[s] = (dot(received, pick) == iota((OBS, OBS), 1).astype(F32)).astype(F32)
        onehot_t[s] = (
            dot_t(pick_t, received) == iota((OBS, OBS), 0).astype(F32)
        ).astype(F32)
        instr = dot(received, jnp.where(row_w == at + 2, 1.0, 0.0))
        corner = jnp.where((row_w == at + 3 + (col_w >> 4)) & (col_w < 64), 1.0, 0.0)
        hit = instr == inst_lane
        spread_w[s] = jnp.where(hit, dot(received, corner), 0.0)
        err_hit = jnp.where(hit & (lane < 16), rinv_row, 0.0)
        inv = jnp.sum(err_hit, axis=1, keepdims=True)
        rinv[s] = jnp.broadcast_to(inv, (OBS, 128))
        obs_z[s] = dot(received, jnp.where(row_w == at + 7, 1.0, 0.0))

    ens_copy.wait()

    def gradient(weights):
        table = dot(onehot_t[0], spread_w[0] * (rinv[0] * weights[0])) + dot(
            onehot_t[1], spread_w[1] * (rinv[1] * weights[1])
        )
        table = table[:CELLS]
        for c in range(4):
            field = dot(table, place[c])
            for t in range(WIN):
                for pr in range(2):
                    at = (t * 2 + pr) * 24
                    grad[t, 2 * pr + c // 2, pl.ds(c % 2, 24, stride=2), :] = field[
                        at : at + 24
                    ]

    def halo_copies(a, k):
        own = reg.at[a, k, pl.ds(ROWS, ROWS), OWN]
        north_rows = reg.at[a, k, pl.ds(0, ROWS), OWN]
        south_rows = reg.at[a, k, pl.ds(2 * ROWS, ROWS), OWN]
        w_strip = strip_send.at[a, k, 0]
        e_strip = strip_send.at[a, k, 1]

        def one(src, dst, slot, i, j):
            return remote(src, dst, hs.at[a, slot, k], hr.at[a, slot, k], i, j)

        always = [
            one(w_strip, strip_recv.at[a, k, 1, 1], 3, lat, west),
            one(e_strip, strip_recv.at[a, k, 0, 1], 2, lat, east),
        ]
        if_n = [
            one(own, south_rows, 1, lat - 1, lon),
            one(w_strip, strip_recv.at[a, k, 1, 2], 7, lat - 1, west),
            one(e_strip, strip_recv.at[a, k, 0, 2], 6, lat - 1, east),
        ]
        if_s = [
            one(own, north_rows, 0, lat + 1, lon),
            one(w_strip, strip_recv.at[a, k, 1, 0], 5, lat + 1, west),
            one(e_strip, strip_recv.at[a, k, 0, 0], 4, lat + 1, east),
        ]
        return always, if_n, if_s

    def start_halo(a, k):
        always, if_n, if_s = halo_copies(a, k)

        @pl.when(has_n)
        def _():
            for c in if_n:
                c.start()

        @pl.when(has_s)
        def _():
            for c in if_s:
                c.start()

        for c in always:
            c.start()

    def wait_halo(a, k):
        always, if_n, if_s = halo_copies(a, k)
        for c in always:
            c.wait_recv()

        @pl.when(has_n)
        def _():
            for c in if_s:
                c.wait_recv()

        @pl.when(has_s)
        def _():
            for c in if_n:
                c.wait_recv()

    def wait_sent(a, k):
        always, if_n, if_s = halo_copies(a, k)
        for c in always:
            c.wait_send()

        @pl.when(has_n)
        def _():
            for c in if_n:
                c.wait_send()

        @pl.when(has_s)
        def _():
            for c in if_s:
                c.wait_send()

    def put_own(a, k, flat):
        for r in range(ROWS):
            row = flat[r * COLS : (r + 1) * COLS]
            reg[a, k, ROWS + r, PAD : PAD + COLS, :] = row
            strip_send[a, k, 0, 4 * r : 4 * r + 4, :] = row[0:4]
            strip_send[a, k, 1, 4 * r : 4 * r + 4, :] = row[COLS - 4 : COLS]

    def send_fields(a):
        def member(k, c):
            summed = ens[k, 0].astype(F32) * grad[0]
            for t in range(1, WIN):
                summed = summed + ens[k, t].astype(F32) * grad[t]
            flat = dot_t(summed.reshape(CELLS, LEV), vert_ref[...])
            put_own(a, k, BETA_ENSEMBLE * flat)
            start_halo(a, k)
            return c

        lax.fori_loop(0, MEM, member, 0)
        summed = (grad[0] + grad[1]) + (grad[2] + grad[3])
        flat = dot_t(summed.reshape(CELLS, LEV), static_ref[...])
        put_own(a, MEM, BETA_STATIC * flat)
        start_halo(a, MEM)

    def smooth(up, mid, down):
        side = pltpu.roll(mid, 1, 0) + pltpu.roll(mid, WIDE - 1, 0)
        return (1.0 - 4.0 * SMOOTH) * mid + SMOOTH * (up + down + side)

    def keep(row, value):
        if row < ROWS:
            return jnp.where(has_n, value, 0.0)
        if row >= 2 * ROWS:
            return jnp.where(has_s, value, 0.0)
        return value

    def spread_twice(a, k):
        for side, col in ((0, PAD - 4), (1, PAD + COLS)):
            for part in range(3):
                for r in range(ROWS):
                    reg[a, k, part * ROWS + r, col : col + 4, :] = strip_recv[
                        a, k, side, part, 4 * r : 4 * r + 4, :
                    ]

        def sweep(read, write, low, high):
            rows = [read(low - 1), read(low)]
            for r in range(low, high):
                rows.append(read(r + 1))
                write(r, keep(r, smooth(rows[0], rows[1], rows[2])))
                rows = rows[1:]

        def to_a(r, v):
            stage_a[r] = v

        def to_b(r, v):
            stage_b[r] = v

        sweep(lambda r: keep(r, reg[a, k, r]), to_a, 1, TALL - 1)
        sweep(lambda r: stage_a[r], to_b, 2, TALL - 2)
        for r in range(ROWS):
            resid[a, k, r] = stage_b[ROWS + r, PAD : PAD + COLS, :]
        sweep(lambda r: stage_b[r], to_a, 3, TALL - 3)
        sweep(lambda r: stage_a[r], to_b, 4, TALL - 4)
        rows = [stage_b[ROWS + r, PAD : PAD + COLS, :] for r in range(ROWS)]
        return jnp.concatenate(rows, axis=0)

    def apply_fields(a, target):
        wait_halo(a, MEM)
        part = BETA_STATIC * dot(spread_twice(a, MEM), static_ref[...])
        part = part.reshape(ROWS, COLS, LEV)
        for t in range(WIN):
            incr[t] = part

        def member(k, c):
            wait_halo(a, k)
            local = BETA_ENSEMBLE * dot(spread_twice(a, k), vert_ref[...])
            local = local.reshape(ROWS, COLS, LEV)
            for t in range(WIN):
                incr[t] += ens[k, t].astype(F32) * local
            return c

        lax.fori_loop(0, MEM, member, 0)
        seen = jnp.zeros((CELLS, 128), F32)
        for c in range(4):
            cells = [
                incr[t, 2 * pr + c // 2, pl.ds(c % 2, 24, stride=2), :]
                for t in range(WIN)
                for pr in range(2)
            ]
            seen = seen + dot_t(jnp.concatenate(cells, axis=0), place[c])
        seen = jnp.concatenate([seen, jnp.zeros((OBS - CELLS, 128), F32)], axis=0)
        for s in range(2):
            value = dot(onehot[s], seen) * spread_w[s]
            value = jnp.sum(value, axis=1, keepdims=True)
            target[s] = jnp.broadcast_to(value, (OBS, 128))

    gradient(obs_z)
    send_fields(0)
    apply_fields(0, obs_e)

    def square(k, c):
        for r in range(ROWS):
            v = resid[0, k, r]
            acc[0] += jnp.sum((v * v).reshape(COLS // 8, 8, LEV), axis=0)
        return c

    lax.fori_loop(0, FIELDS, square, 0)
    sum_a = total(acc[0])
    sum_b = jnp.zeros((1, 1), F32)
    for s in range(2):
        e = obs_e[s]
        sum_b = sum_b + jnp.sum(rinv[s] * e * e, axis=0, keepdims=True)[:, 0:1]
    lane1 = iota((1, 128), 1)
    red_a_send[...] = jnp.where(lane1 == 0, sum_a, 0.0) + jnp.where(lane1 == 1, sum_b, 0.0)

    block_to_lat(red_a_send, red_a, ras, rar)
    gradient(obs_e)
    send_fields(1)
    end_lat(red_a_send, red_a, ras, rar)
    part = red_a[0]
    for i in range(1, NLAT):
        part = part + red_a[i]
    red_b_send[...] = part
    rows_to_lon(red_b_send, red_b, rbs, rbr, True)
    apply_fields(1, obs_z)
    end_lon(red_b_send, red_b, rbs, rbr, True)
    whole = red_b[0]
    for j in range(1, NLON):
        whole = whole + red_b[j]
    a0 = whole[:, 0:1]
    b0 = whole[:, 1:2]
    step0 = a0 / (a0 + b0)

    acc[...] = jnp.zeros_like(acc)

    def next_residual(k, c):
        for r in range(ROWS):
            r0 = resid[0, k, r]
            r1 = (1.0 - step0) * r0 - step0 * resid[1, k, r]
            resid[1, k, r] = r1
            acc[0] += jnp.sum((r1 * r1).reshape(COLS // 8, 8, LEV), axis=0)
            acc[1] += jnp.sum((r1 * r0).reshape(COLS // 8, 8, LEV), axis=0)
        return c

    lax.fori_loop(0, FIELDS, next_residual, 0)
    partial = [total(acc[0]), total(acc[1])]
    sum_v = jnp.zeros((1, 1), F32)
    sum_w = jnp.zeros((1, 1), F32)
    blocks = jnp.zeros((OBS, 128), F32)
    word = lane & 15
    for s in range(2):
        e = obs_e[s]
        nxt = (1.0 - step0) * e - step0 * obs_z[s]
        sum_v = sum_v + jnp.sum(rinv[s] * nxt * nxt, axis=0, keepdims=True)[:, 0:1]
        sum_w = sum_w + jnp.sum(rinv[s] * nxt * e, axis=0, keepdims=True)[:, 0:1]
        blocks = jnp.where(word == s, e, blocks)
        blocks = jnp.where(word == 2 + s, nxt, blocks)
    partial = partial + [sum_v, sum_w]
    for n in range(4):
        blocks = jnp.where(word == 4 + n, partial[n], blocks)
    blocks = jnp.where((lane >> 4) == (iota((OBS, 128), 0) >> 5), blocks, 0.0)
    out_rows = blocks[0:NLON]
    for i in range(1, NLAT):
        out_rows = out_rows + blocks[i * NLON : (i + 1) * NLON]
    for j in range(NLON):
        send2[j] = out_rows[j : j + 1, :]

    back = exchange(send2, first2, flat2, second2, x2s, x2r, y2s, y2r)
    sums = jnp.sum(back, axis=0, keepdims=True)
    got = [
        jnp.sum(jnp.where(lane1 == base + 4 + n, sums, 0.0), axis=1, keepdims=True)
        for n in range(4)
    ]
    rr1, u, v, w = got
    ratio = rr1 / a0
    below = (rr1 + 2.0 * ratio * u + ratio * ratio * a0) + (
        v + 2.0 * ratio * w + ratio * ratio * b0
    )
    step1 = rr1 / below
    c0 = step0 + step1 * ratio
    c1 = step1

    def finish(k, c):
        for r in range(ROWS):
            out_member[k, r] = c0 * resid[0, k, r] + c1 * resid[1, k, r]
        return c

    lax.fori_loop(0, MEM, finish, 0)
    for r in range(ROWS):
        out_static[r] = c0 * resid[0, MEM, r] + c1 * resid[1, MEM, r]

    mine = dest_row == iota((OBS, OBS), 0)
    equiv = jnp.zeros((1, OBS), F32)
    for s in range(2):
        mix = jnp.where(lane1 == base + s, c0, 0.0) + jnp.where(lane1 == base + 2 + s, c1, 0.0)
        value = jnp.sum(back * mix, axis=1, keepdims=True)
        chosen = jnp.where(mine & (rank == float(s)), value, 0.0)
        equiv = equiv + jnp.sum(chosen, axis=0, keepdims=True)
    out_equiv[...] = equiv

    def drain(k, c):
        wait_sent(0, k)
        wait_sent(1, k)
        return c

    lax.fori_loop(0, FIELDS, drain, 0)


def body(
    ensemble, vert_loc, static_vert, inst_vert, inst_err, obs_dest, obs_patch,
    obs_window, obs_inst, obs_hweight, innovation, obs_count,
):
    vmem = pl.BlockSpec(memory_space=pltpu.VMEM)
    dma = pltpu.SemaphoreType.DMA
    scratch = [
        pltpu.VMEM((MEM, WIN, ROWS, COLS, LEV), jnp.bfloat16),
        pltpu.VMEM((NLON, 1, 128), F32),
        pltpu.VMEM((NLON, 1, 128), F32),
        pltpu.VMEM((NLON, 128), F32),
        pltpu.VMEM((NLAT, NLON, 128), F32),
        pltpu.VMEM((NLON, 1, 128), F32),
        pltpu.VMEM((NLON, 1, 128), F32),
        pltpu.VMEM((NLON, 128), F32),
        pltpu.VMEM((NLAT, NLON, 128), F32),
        pltpu.VMEM((1, 128), F32),
        pltpu.VMEM((NLAT, 1, 128), F32),
        pltpu.VMEM((1, 128), F32),
        pltpu.VMEM((NLON, 1, 128), F32),
        pltpu.VMEM((4, 128, LEV), F32),
        pltpu.VMEM((2, OBS, OBS), F32),
        pltpu.VMEM((2, OBS, OBS), F32),
        pltpu.VMEM((2, OBS, 128), F32),
        pltpu.VMEM((2, OBS, 128), F32),
        pltpu.VMEM((2, OBS, 128), F32),
        pltpu.VMEM((2, OBS, 128), F32),
        pltpu.VMEM((WIN, ROWS, COLS, LEV), F32),
        pltpu.VMEM((WIN, ROWS, COLS, LEV), F32),
        pltpu.VMEM((2, FIELDS, TALL, WIDE, LEV), F32),
        pltpu.VMEM((2, FIELDS, 2, 16, LEV), F32),
        pltpu.VMEM((2, FIELDS, 2, 3, 16, LEV), F32),
        pltpu.VMEM((TALL, WIDE, LEV), F32),
        pltpu.VMEM((TALL, WIDE, LEV), F32),
        pltpu.VMEM((2, FIELDS, ROWS, COLS, LEV), F32),
        pltpu.VMEM((2, 8, LEV), F32),
        dma(()),
        dma((NLON,)), dma((NLON,)), dma((NLAT,)), dma((NLAT,)),
        dma((NLON,)), dma((NLON,)), dma((NLAT,)), dma((NLAT,)),
        dma((NLAT,)), dma((NLAT,)), dma((NLON,)), dma((NLON,)),
        dma((2, 8, FIELDS)), dma((2, 8, FIELDS)),
    ]
    static_out, member_out, equiv = pl.pallas_call(
        kernel,
        out_shape=(
            jax.ShapeDtypeStruct((ROWS, COLS, LEV), F32),
            jax.ShapeDtypeStruct((MEM, ROWS, COLS, LEV), F32),
            jax.ShapeDtypeStruct((1, OBS), F32),
        ),
        in_specs=[pl.BlockSpec(memory_space=pl.ANY)] + [vmem] * 12,
        out_specs=(vmem, vmem, vmem),
        scratch_shapes=scratch,
        compiler_params=pltpu.CompilerParams(
            collective_id=0, has_side_effects=True, vmem_limit_bytes=56 << 20
        ),
        name="inner_loop",
    )(
        ensemble, vert_loc, static_vert, inst_vert,
        jnp.tile(inst_err, 8).reshape(1, 128),
        obs_dest, obs_dest.reshape(1, OBS), obs_patch.reshape(1, OBS),
        obs_window.reshape(1, OBS), obs_inst.reshape(1, OBS), obs_hweight,
        innovation.reshape(1, OBS), obs_count.reshape(1, 1),
    )
    return static_out, member_out, equiv.reshape(OBS)


def solution(mesh):
    both = ("lat", "lon")
    in_specs = (
        P(None, None, "lat", "lon", None), P(), P(), P(), P(), P(both, None),
        P(both), P(both), P(both), P(None, both), P(both), P(both),
    )
    out_specs = (P("lat", "lon", None), P(None, "lat", "lon", None), P(both))
    return jax.shard_map(
        body, mesh=mesh, in_specs=in_specs, out_specs=out_specs, check_vma=False
    )
```

```python
import jax
import jax.numpy as jnp
from jax import lax
from jax.experimental import pallas as pl
from jax.experimental.pallas import tpu as pltpu
from jax.sharding import PartitionSpec as P

F32 = jnp.float32
BF16 = jnp.bfloat16
MESH = pl.DeviceIdType.MESH
SMOOTH = 0.15
BETA_STATIC = 0.5
BETA_ENSEMBLE = 0.85
NLAT, NLON = 8, 32
MEM, WIN, ROWS, COLS, LEV, NINST = 8, 4, 4, 48, 128, 16
FIELDS = MEM + 1
CELLS = ROWS * COLS
OBS = 256
SLOTS = 2 * OBS
PAD = 8
WIDE = COLS + 2 * PAD
TALL = 3 * ROWS
OWN = pl.ds(PAD, COLS)


def dot(a, b, precision=None):
    return lax.dot_general(
        a, b, (((1,), (0,)), ((), ())), precision=precision, preferred_element_type=F32
    )


def dot_t(a, b, precision=None):
    return lax.dot_general(
        a, b, (((1,), (1,)), ((), ())), precision=precision, preferred_element_type=F32
    )


def split(x):
    high = x.astype(BF16)
    return high, (x - high.astype(F32)).astype(BF16)


def dot3(x, w_high, w_low):
    high, low = split(x)
    return dot(high, w_high) + (dot(low, w_high) + dot(high, w_low))


def pick_rows(onehot, x):
    high, low = split(x)
    return dot(onehot, high) + dot(onehot, low)


def iota(shape, dim):
    return lax.broadcasted_iota(jnp.int32, shape, dim)


def total(x):
    return jnp.sum(jnp.sum(x, axis=1, keepdims=True), axis=0, keepdims=True)


def fold(x):
    return jnp.sum(x.reshape(COLS // 8, 8, LEV), axis=0)


def kernel(
    count_ref, ens_hbm, vert_hbm, static_hbm, inst_hbm, err_hbm, dest_hbm,
    patch_hbm, window_hbm, instr_hbm, hweight_hbm, innov_hbm,
    out_fields, out_coef, out_equiv,
    ens, vert_ref, static_ref, inst_ref, err_ref, dest_ref,
    patch_ref, window_ref, instr_ref, hweight_ref, innov_ref,
    err_wide, send1, first1, block1, second1, send2, first2, block2, second2, arrived,
    red_a_send, red_a, red_b_send, red_b,
    level_w, place_f, place_w, place_wt, onehot, onehot_t, spread_w, rinv, obs_e, obs_z,
    grad, incr, reg, strip_send, strip_recv, corner_send, corner_recv, tally, stage_a, stage_b, resid, acc,
    in_sem, ens_sem, out_sem, x1, y1, x2, y2, ra, rb, hs, hr,
):
    lat = lax.axis_index("lat")
    lon = lax.axis_index("lon")
    has_n = lat > 0
    has_s = lat < NLAT - 1
    west = lax.rem(lon + NLON - 1, NLON)
    east = lax.rem(lon + 1, NLON)

    barrier = pltpu.get_barrier_semaphore()

    def greet(i, j):
        pl.semaphore_signal(barrier, inc=1, device_id=(i, j), device_id_type=MESH)

    def greet_lon(d, c):
        greet(lat, lax.rem(lon + d, NLON))
        return c

    def greet_lat(d, c):
        greet(lax.rem(lat + d, NLAT), lon)
        return c

    small = [
        (dest_hbm, dest_ref), (patch_hbm, patch_ref), (window_hbm, window_ref),
        (instr_hbm, instr_ref), (hweight_hbm, hweight_ref), (innov_hbm, innov_ref),
        (vert_hbm, vert_ref), (static_hbm, static_ref), (inst_hbm, inst_ref),
        (err_hbm, err_ref),
    ]
    loads = [
        pltpu.make_async_copy(a, b, in_sem.at[n]) for n, (a, b) in enumerate(small)
    ]
    for c in loads:
        c.start()
    lax.fori_loop(1, NLON, greet_lon, 0)
    lax.fori_loop(1, NLAT, greet_lat, 0)
    for step in (1, NLAT - 1):
        greet(lax.rem(lat + step, NLAT), west)
        greet(lax.rem(lat + step, NLAT), east)
    ens_copy = pltpu.make_async_copy(ens_hbm, ens, ens_sem)
    ens_copy.start()
    for c in loads:
        c.wait()

    dest_row = dest_ref[...]
    square0 = iota((OBS, OBS), 0)
    square1 = iota((OBS, OBS), 1)
    dest_f = jnp.where(square0 == square1, dest_row.astype(F32), 0.0)
    dest_col = jnp.sum(dest_f, axis=1, keepdims=True)
    same = (dest_col == dest_row.astype(F32)) & (square0 < square1)
    rank = jnp.sum(same.astype(F32), axis=0, keepdims=True)
    group = (7 - (dest_row >> 5)) * 2 + rank.astype(jnp.int32)
    active = (iota((1, OBS), 1) < count_ref[0]).astype(F32)
    words = jnp.concatenate(
        [
            patch_ref[...].astype(F32),
            window_ref[...].astype(F32),
            instr_ref[...].astype(F32),
            hweight_ref[...] * active,
            innov_ref[...],
        ],
        axis=0,
    )
    tiled = jnp.concatenate([words] * 16, axis=0)
    tiled = jnp.where((iota((128, OBS), 0) >> 3) == group, tiled, 0.0)
    to_lon = (iota((NLON, OBS), 0) == (dest_row & 31)).astype(F32)
    outgoing = dot_t(to_lon, tiled, lax.Precision.HIGHEST)
    for j in range(NLON):
        send1[j] = outgoing[j : j + 1, :]

    err_wide[...] = jnp.ones_like(err_wide)
    err_wide[:, 0:NINST] = err_ref[...]
    for n, ref in enumerate((vert_ref, static_ref)):
        w = ref[...]
        level_w[n, 0], level_w[n, 1] = split(w)
        level_w[n, 2], level_w[n, 3] = split(w.T)
    place_f[...] = jnp.zeros_like(place_f)
    for c in range(4):
        place_f[16 * c : 16 * c + 16, LEV * c : LEV * c + LEV] = inst_ref[...]
    for n, half in enumerate(split(place_f[...])):
        place_w[n] = half
    for c in range(4):
        for n, half in enumerate(split(place_f[:, LEV * c : LEV * c + LEV].T)):
            place_wt[n, LEV * c : LEV * c + LEV, :] = half
    for a in range(2):
        reg[a, :, :, 0:PAD, :] = jnp.zeros((FIELDS, TALL, PAD, LEV), F32)
        reg[a, :, :, PAD + COLS : WIDE, :] = jnp.zeros((FIELDS, TALL, PAD, LEV), F32)
    acc[...] = jnp.zeros_like(acc)
    incr[...] = jnp.zeros_like(incr)

    pl.semaphore_wait(barrier, NLON - 1 + NLAT - 1 + 4)

    def remote(src, dst, ssem, rsem, i, j):
        return pltpu.make_async_remote_copy(
            src_ref=src, dst_ref=dst, send_sem=ssem, recv_sem=rsem,
            device_id=(i, j), device_id_type=MESH,
        )

    def rows_done(rows, ssem, rsem):
        ref = tally.at[pl.ds(0, rows)]
        return remote(ref, ref, ssem, rsem, lat, east)

    def rows_to_lon(send, first, sems, one_row):
        def go(d, c):
            j = lax.rem(lon + d, NLON)
            src = send if one_row else send.at[j]
            remote(src, first.at[lon], sems.at[0], sems.at[1], lat, j).start()
            return c

        lax.fori_loop(1, NLON, go, 0)
        first[lon] = send[...] if one_row else send[lon]

    def all_lon(sems):
        return rows_done(NLON - 1, sems.at[0], sems.at[1])

    def block_to_lat(send, second, sems, whole):
        def go(d, c):
            i = lax.rem(lat + d, NLAT)
            src = send if whole else send.at[i]
            remote(src, second.at[lat], sems.at[0], sems.at[1], i, lon).start()
            return c

        lax.fori_loop(1, NLAT, go, 0)
        second[lat] = send[...] if whole else send[lat]

    def all_lat(sems, rows):
        return rows_done((NLAT - 1) * rows, sems.at[0], sems.at[1])

    lanes8 = iota((8, 128), 1) >> 4

    def exchange(send, first, block, second, xs, ys):
        rows_to_lon(send, first, xs, False)
        all_lon(xs).wait_recv()
        for q in range(4):
            swapped = jnp.zeros((8, 128), F32)
            for n in range(8):
                row = jnp.broadcast_to(first[8 * q + n], (8, 128))
                row = pltpu.roll(row, 0, 1, stride=16, stride_axis=0)
                if n > 0:
                    row = pltpu.roll(row, 128 - 16 * n, 1)
                swapped = jnp.where(lanes8 == 7 - n, row, swapped)
            for i in range(NLAT):
                block[i, q : q + 1, :] = swapped[i : i + 1, :]
        block_to_lat(block, second, ys, False)
        all_lat(ys, 4).wait_recv()
        for i in range(NLAT):
            for q in range(4):
                row = jnp.broadcast_to(second[i, q : q + 1, :], (8, 128))
                row = pltpu.roll(row, 16, 1, stride=16, stride_axis=0)
                at = (i * 4 + q) * 8
                arrived[at : at + 8, :] = row
        return arrived[...]

    received = exchange(send1, first1, block1, second1, x1, y1)

    lane = iota((OBS, 128), 1)
    inst_lane = (lane & 15).astype(F32)
    err_row = err_wide[...]
    rinv_row = 1.0 / (err_row * err_row)
    row_w = iota((128, 128), 0)
    col_w = iota((128, 128), 1)
    ids = received.astype(BF16)
    for s in range(2):
        at = 8 * s
        here = slice(s * OBS, (s + 1) * OBS)
        l0 = iota((128, OBS), 0)
        pick = jnp.where(l0 == at, 1.0, 0.0) + jnp.where(l0 == at + 1, 48.0, 0.0)
        l1 = iota((OBS, 128), 1)
        pick_t = jnp.where(l1 == at, 1.0, 0.0) + jnp.where(l1 == at + 1, 48.0, 0.0)
        hot = dot(ids, pick.astype(BF16)) == square1.astype(F32)
        onehot[here, :] = hot.astype(F32).astype(BF16)
        hot_t = dot_t(pick_t.astype(BF16), ids) == square0.astype(F32)
        onehot_t[:, here] = hot_t.astype(F32).astype(BF16)
        instr = dot(ids, jnp.where(row_w == at + 2, 1.0, 0.0).astype(BF16))
        corner = jnp.where((row_w == at + 3 + (col_w >> 4)) & (col_w < 64), 1.0, 0.0)
        hit = instr == inst_lane
        chosen = dot(received, corner, lax.Precision.HIGHEST)
        spread_w[here, :] = jnp.where(hit, chosen, 0.0)
        err_hit = jnp.where(hit & (lane < 16), rinv_row, 0.0)
        inv = jnp.sum(err_hit, axis=1, keepdims=True)
        rinv[here, :] = jnp.broadcast_to(inv, (OBS, 128))
        obs_z[here, :] = jnp.broadcast_to(received[:, at + 7 : at + 8], (OBS, 128))

    ens_copy.wait()

    def gradient(weights):
        table = pick_rows(onehot_t[...], spread_w[...] * (rinv[...] * weights[...]))
        table = table[:CELLS]
        for h in range(2):
            wide = slice(h * 2 * LEV, (h + 1) * 2 * LEV)
            both = dot3(table, place_w[0, :, wide], place_w[1, :, wide])
            for c2 in range(2):
                field = both[:, c2 * LEV : (c2 + 1) * LEV]
                for t in range(WIN):
                    for pr in range(2):
                        at = (t * 2 + pr) * 24
                        grad[t, 2 * pr + h, pl.ds(c2, 24, stride=2), :] = field[
                            at : at + 24
                        ]

    def halo_copies(a, k):
        own = reg.at[a, k, pl.ds(ROWS, ROWS), OWN]
        north_rows = reg.at[a, k, pl.ds(0, ROWS), OWN]
        south_rows = reg.at[a, k, pl.ds(2 * ROWS, ROWS), OWN]
        w_strip = strip_send.at[a, k, 0]
        e_strip = strip_send.at[a, k, 1]

        def one(src, dst, part, i, j):
            return remote(src, dst, hs.at[a, part], hr.at[a, part, k], i, j)

        def corner(n, m):
            return corner_send.at[a, k, n], corner_recv.at[a, k, m]

        always = [
            one(w_strip, strip_recv.at[a, k, 1], 0, lat, west),
            one(e_strip, strip_recv.at[a, k, 0], 0, lat, east),
        ]
        to_n = [
            one(own, south_rows, 2, lat - 1, lon),
            one(*corner(0, 3), 2, lat - 1, west),
            one(*corner(1, 2), 2, lat - 1, east),
        ]
        to_s = [
            one(own, north_rows, 1, lat + 1, lon),
            one(*corner(2, 1), 1, lat + 1, west),
            one(*corner(3, 0), 1, lat + 1, east),
        ]
        return always, to_n, to_s

    def start_halo(a, k):
        always, to_n, to_s = halo_copies(a, k)

        @pl.when(has_n)
        def _():
            for c in to_n:
                c.start()

        @pl.when(has_s)
        def _():
            for c in to_s:
                c.start()

        for c in always:
            c.start()

    def wait_halo(a, k):
        rows_done(32, hs.at[a, 0], hr.at[a, 0, k]).wait_recv()

        @pl.when(has_n)
        def _():
            rows_done(CELLS + 16, hs.at[a, 1], hr.at[a, 1, k]).wait_recv()

        @pl.when(has_s)
        def _():
            rows_done(CELLS + 16, hs.at[a, 2], hr.at[a, 2, k]).wait_recv()

    def sent_halo(a):
        rows_done(FIELDS * 32, hs.at[a, 0], hr.at[a, 0, 0]).wait_send()

        @pl.when(has_s)
        def _():
            rows_done(FIELDS * (CELLS + 16), hs.at[a, 1], hr.at[a, 1, 0]).wait_send()

        @pl.when(has_n)
        def _():
            rows_done(FIELDS * (CELLS + 16), hs.at[a, 2], hr.at[a, 2, 0]).wait_send()

    def put_own(a, k, flat):
        for r in range(ROWS):
            row = flat[r * COLS : (r + 1) * COLS]
            reg[a, k, ROWS + r, PAD : PAD + COLS, :] = row
            strip_send[a, k, 0, 4 * r : 4 * r + 4, :] = row[0:4]
            strip_send[a, k, 1, 4 * r : 4 * r + 4, :] = row[COLS - 4 : COLS]
            for south in range(2):
                near = ROWS - 1 - r if south else r
                if near < 3:
                    at = (0, 3, 5)[near]
                    n = 3 - near
                    corner_send[a, k, 2 * south, at : at + n, :] = row[0:n]
                    corner_send[a, k, 2 * south + 1, at : at + n, :] = row[COLS - n : COLS]

    def send_fields(a):
        def member(k, c):
            summed = ens[k, 0].astype(F32) * grad[0]
            for t in range(1, WIN):
                summed = summed + ens[k, t].astype(F32) * grad[t]
            flat = dot3(summed.reshape(CELLS, LEV), level_w[0, 2], level_w[0, 3])
            put_own(a, k, BETA_ENSEMBLE * flat)
            start_halo(a, k)
            return c

        lax.fori_loop(0, MEM, member, 0)
        summed = (grad[0] + grad[1]) + (grad[2] + grad[3])
        flat = dot3(summed.reshape(CELLS, LEV), level_w[1, 2], level_w[1, 3])
        put_own(a, MEM, BETA_STATIC * flat)
        start_halo(a, MEM)

    def smooth(up, mid, down):
        side = pltpu.roll(mid, 1, 0) + pltpu.roll(mid, WIDE - 1, 0)
        return (1.0 - 4.0 * SMOOTH) * mid + SMOOTH * (up + down + side)

    def keep(row, value):
        if row < ROWS:
            return jnp.where(has_n, value, 0.0)
        if row >= 2 * ROWS:
            return jnp.where(has_s, value, 0.0)
        return value

    def spread_twice(a, k, note):
        for side, col in ((0, PAD - 4), (1, PAD + COLS)):
            for r in range(ROWS):
                reg[a, k, ROWS + r, col : col + 4, :] = strip_recv[
                    a, k, side, 4 * r : 4 * r + 4, :
                ]
            for south in range(2):
                for near in range(3):
                    at = (0, 3, 5)[near]
                    n = 3 - near
                    row = 2 * ROWS + near if south else ROWS - 1 - near
                    first_col = PAD + COLS if side else PAD - n
                    reg[a, k, row, first_col : first_col + n, :] = corner_recv[
                        a, k, 2 * south + side, at : at + n, :
                    ]

        def sweep(read, write, low, high):
            rows = [read(low - 1), read(low)]
            for r in range(low, high):
                rows.append(read(r + 1))
                write(r, keep(r, smooth(rows[0], rows[1], rows[2])))
                rows = rows[1:]

        def to_a(r, v):
            stage_a[r] = v

        def to_b(r, v):
            stage_b[r] = v

        sweep(lambda r: keep(r, reg[a, k, r]), to_a, 1, TALL - 1)
        sweep(lambda r: stage_a[r], to_b, 2, TALL - 2)
        for r in range(ROWS):
            note(k, r, stage_b[ROWS + r, PAD : PAD + COLS, :])
        sweep(lambda r: stage_b[r], to_a, 3, TALL - 3)
        sweep(lambda r: stage_a[r], to_b, 4, TALL - 4)
        rows = [stage_b[ROWS + r, PAD : PAD + COLS, :] for r in range(ROWS)]
        return jnp.concatenate(rows, axis=0)

    def apply_fields(a, target, note):
        def member(k, c):
            wait_halo(a, k)
            local = dot3(spread_twice(a, k, note), level_w[0, 0], level_w[0, 1])
            local = (BETA_ENSEMBLE * local).reshape(ROWS, COLS, LEV)
            for t in range(WIN):
                incr[t] += ens[k, t].astype(F32) * local
            return c

        lax.fori_loop(0, MEM, member, 0)
        wait_halo(a, MEM)
        part = dot3(spread_twice(a, MEM, note), level_w[1, 0], level_w[1, 1])
        part = (BETA_STATIC * part).reshape(ROWS, COLS, LEV)
        for t in range(WIN):
            incr[t] += part
        seen = jnp.zeros((CELLS, 128), F32)
        for h in range(2):
            pair = []
            for c2 in range(2):
                cells = [
                    incr[t, 2 * pr + h, pl.ds(c2, 24, stride=2), :]
                    for t in range(WIN)
                    for pr in range(2)
                ]
                pair.append(jnp.concatenate(cells, axis=0))
            tall = slice(h * 2 * LEV, (h + 1) * 2 * LEV)
            seen = seen + dot3(
                jnp.concatenate(pair, axis=1), place_wt[0, tall, :], place_wt[1, tall, :]
            )
        seen = jnp.concatenate([seen, jnp.zeros((OBS - CELLS, 128), F32)], axis=0)
        value = pick_rows(onehot[...], seen) * spread_w[...]
        value = jnp.sum(value, axis=1, keepdims=True)
        target[...] = jnp.broadcast_to(value, (SLOTS, 128))

    def note_first(k, r, v):
        resid[0, k, r] = v
        acc[0] += fold(v * v)

    gradient(obs_z)
    send_fields(0)
    apply_fields(0, obs_e, note_first)
    out0 = pltpu.make_async_copy(resid.at[0], out_fields.at[0], out_sem.at[0])
    out0.start()
    sum_a = total(acc[0])
    first_e = obs_e[...]
    sum_b = jnp.sum(rinv[...] * first_e * first_e, axis=0, keepdims=True)[:, 0:1]
    lane1 = iota((1, 128), 1)
    red_a_send[...] = jnp.where(lane1 == 0, sum_a, 0.0) + jnp.where(lane1 == 1, sum_b, 0.0)
    block_to_lat(red_a_send, red_a, ra, True)

    incr[...] = jnp.zeros_like(incr)
    acc[...] = jnp.zeros_like(acc)
    gradient(obs_e)
    send_fields(1)
    all_lat(ra, 1).wait_recv()
    part = red_a[0]
    for i in range(1, NLAT):
        part = part + red_a[i]
    red_b_send[...] = part
    rows_to_lon(red_b_send, red_b, rb, True)
    all_lon(rb).wait_recv()
    whole = red_b[0]
    for j in range(1, NLON):
        whole = whole + red_b[j]
    a0 = whole[:, 0:1]
    b0 = whole[:, 1:2]
    step0 = a0 / (a0 + b0)
    rest0 = b0 / (a0 + b0)

    def note_second(k, r, v):
        r0 = resid[0, k, r]
        r1 = rest0 * r0 - step0 * v
        resid[1, k, r] = r1
        acc[0] += fold(r1 * r1)
        acc[1] += fold(r1 * r0)

    apply_fields(1, obs_z, note_second)
    out1 = pltpu.make_async_copy(resid.at[1], out_fields.at[1], out_sem.at[1])
    out1.start()

    partial = [total(acc[0]), total(acc[1])]
    sum_v = jnp.zeros((1, 1), F32)
    sum_w = jnp.zeros((1, 1), F32)
    blocks = jnp.zeros((OBS, 128), F32)
    word = lane & 15
    for s in range(2):
        here = slice(s * OBS, (s + 1) * OBS)
        e = obs_e[here, :]
        nxt = rest0 * e - step0 * obs_z[here, :]
        weighted = rinv[here, :] * nxt
        sum_v = sum_v + jnp.sum(weighted * nxt, axis=0, keepdims=True)[:, 0:1]
        sum_w = sum_w + jnp.sum(weighted * e, axis=0, keepdims=True)[:, 0:1]
        blocks = jnp.where(word == s, e, blocks)
        blocks = jnp.where(word == 2 + s, nxt, blocks)
    partial = partial + [sum_v, sum_w]
    for n in range(4):
        blocks = jnp.where(word == 4 + n, partial[n], blocks)
    blocks = jnp.where((lane >> 4) == 7 - (iota((OBS, 128), 0) >> 5), blocks, 0.0)
    out_rows = blocks[0:NLON]
    for i in range(1, NLAT):
        out_rows = out_rows + blocks[i * NLON : (i + 1) * NLON]
    for j in range(NLON):
        send2[j] = out_rows[j : j + 1, :]

    back = exchange(send2, first2, block2, second2, x2, y2)
    sums = jnp.sum(back, axis=0, keepdims=True)
    rr1, u, v, w = [sums[:, 4 + n : 5 + n] for n in range(4)]
    ratio = rr1 / a0
    below = (rr1 + 2.0 * ratio * u + ratio * ratio * a0) + (
        v + 2.0 * ratio * w + ratio * ratio * b0
    )
    step1 = rr1 / below
    c0 = step0 + step1 * ratio
    c1 = step1
    out_coef[...] = jnp.where(iota((2, 128), 0) == 0, c0, c1)

    mine = dest_row == square0
    equiv = jnp.zeros((1, OBS), F32)
    for s in range(2):
        value = c0 * back[:, s : s + 1] + c1 * back[:, 2 + s : 3 + s]
        chosen = jnp.where(mine & (rank == float(s)), value, 0.0)
        equiv = equiv + jnp.sum(chosen, axis=0, keepdims=True)
    out_equiv[...] = equiv

    out0.wait()
    out1.wait()
    for sems in (x1, x2, rb):
        all_lon(sems).wait_send()
    for sems, rows in ((y1, 4), (y2, 4), (ra, 1)):
        all_lat(sems, rows).wait_send()
    sent_halo(0)
    sent_halo(1)


def finish(fields, coef, equiv, out_static, out_member, out_equiv, held, made, sem_in, sem_out):
    loads = [
        [pltpu.make_async_copy(fields.at[a, k], held.at[a, k], sem_in.at[a, k]) for a in range(2)]
        for k in range(FIELDS)
    ]
    for pair in loads:
        for c in pair:
            c.start()
    out_equiv[...] = equiv[...]
    c0 = coef[0:1, :]
    c1 = coef[1:2, :]
    stores = []
    for k in range(FIELDS):
        for c in loads[k]:
            c.wait()
        for r in range(ROWS):
            made[k, r] = c0 * held[0, k, r] + c1 * held[1, k, r]
        target = out_static if k == MEM else out_member.at[k]
        stores.append(pltpu.make_async_copy(made.at[k], target, sem_out.at[k]))
        stores[-1].start()
    for c in stores:
        c.wait()


def body(
    ensemble, vert_loc, static_vert, inst_vert, inst_err, obs_dest, obs_patch,
    obs_window, obs_inst, obs_hweight, innovation, obs_count,
):
    vmem = pl.BlockSpec(memory_space=pltpu.VMEM)
    anywhere = pl.BlockSpec(memory_space=pl.ANY)
    hbm = pl.BlockSpec(memory_space=pltpu.HBM)
    dma = pltpu.SemaphoreType.DMA
    ints = jnp.int32
    exchange = [
        pltpu.VMEM((NLON, 1, 128), F32),
        pltpu.VMEM((NLON, 1, 128), F32),
        pltpu.VMEM((NLAT, 4, 128), F32),
        pltpu.VMEM((NLAT, 4, 128), F32),
    ]
    scratch = [
        pltpu.VMEM((MEM, WIN, ROWS, COLS, LEV), BF16),
        pltpu.VMEM((LEV, LEV), F32),
        pltpu.VMEM((LEV, LEV), F32),
        pltpu.VMEM((NINST, LEV), F32),
        pltpu.VMEM((1, NINST), F32),
        pltpu.VMEM((1, OBS), ints),
        pltpu.VMEM((1, OBS), ints),
        pltpu.VMEM((1, OBS), ints),
        pltpu.VMEM((1, OBS), ints),
        pltpu.VMEM((4, OBS), F32),
        pltpu.VMEM((1, OBS), F32),
        pltpu.VMEM((1, 128), F32),
        *exchange,
        *exchange,
        pltpu.VMEM((OBS, 128), F32),
        pltpu.VMEM((1, 128), F32),
        pltpu.VMEM((NLAT, 1, 128), F32),
        pltpu.VMEM((1, 128), F32),
        pltpu.VMEM((NLON, 1, 128), F32),
        pltpu.VMEM((2, 4, LEV, LEV), BF16),
        pltpu.VMEM((128, 4 * LEV), F32),
        pltpu.VMEM((2, 128, 4 * LEV), BF16),
        pltpu.VMEM((2, 4 * LEV, 128), BF16),
        pltpu.VMEM((SLOTS, OBS), BF16),
        pltpu.VMEM((OBS, SLOTS), BF16),
        pltpu.VMEM((SLOTS, 128), F32),
        pltpu.VMEM((SLOTS, 128), F32),
        pltpu.VMEM((SLOTS, 128), F32),
        pltpu.VMEM((SLOTS, 128), F32),
        pltpu.VMEM((WIN, ROWS, COLS, LEV), F32),
        pltpu.VMEM((WIN, ROWS, COLS, LEV), F32),
        pltpu.VMEM((2, FIELDS, TALL, WIDE, LEV), F32),
        pltpu.VMEM((2, FIELDS, 2, 16, LEV), F32),
        pltpu.VMEM((2, FIELDS, 2, 16, LEV), F32),
        pltpu.VMEM((2, FIELDS, 4, 8, LEV), F32),
        pltpu.VMEM((2, FIELDS, 4, 8, LEV), F32),
        pltpu.VMEM((FIELDS * (CELLS + 16), 128), F32),
        pltpu.VMEM((TALL, WIDE, LEV), F32),
        pltpu.VMEM((TALL, WIDE, LEV), F32),
        pltpu.VMEM((2, FIELDS, ROWS, COLS, LEV), F32),
        pltpu.VMEM((2, 8, LEV), F32),
        dma((10,)), dma(()), dma((2,)),
        dma((2,)), dma((2,)), dma((2,)), dma((2,)), dma((2,)), dma((2,)),
        dma((2, 3)), dma((2, 3, FIELDS)),
    ]
    fields, coef, equiv = pl.pallas_call(
        kernel,
        out_shape=(
            jax.ShapeDtypeStruct((2, FIELDS, ROWS, COLS, LEV), F32),
            jax.ShapeDtypeStruct((2, 128), F32),
            jax.ShapeDtypeStruct((1, OBS), F32),
        ),
        in_specs=[pl.BlockSpec(memory_space=pltpu.SMEM)] + [hbm] * 11,
        out_specs=(anywhere, vmem, vmem),
        scratch_shapes=scratch,
        compiler_params=pltpu.CompilerParams(
            collective_id=0, has_side_effects=True, vmem_limit_bytes=67043328
        ),
        name="inner_loop",
    )(
        obs_count, ensemble, vert_loc, static_vert, inst_vert,
        inst_err.reshape(1, NINST), obs_dest.reshape(1, OBS),
        obs_patch.reshape(1, OBS), obs_window.reshape(1, OBS),
        obs_inst.reshape(1, OBS), obs_hweight, innovation.reshape(1, OBS),
    )
    static, member, equiv = pl.pallas_call(
        finish,
        out_shape=(
            jax.ShapeDtypeStruct((ROWS, COLS, LEV), F32),
            jax.ShapeDtypeStruct((MEM, ROWS, COLS, LEV), F32),
            jax.ShapeDtypeStruct((1, OBS), F32),
        ),
        in_specs=[hbm, vmem, vmem],
        out_specs=(hbm, hbm, vmem),
        scratch_shapes=[
            pltpu.VMEM((2, FIELDS, ROWS, COLS, LEV), F32),
            pltpu.VMEM((FIELDS, ROWS, COLS, LEV), F32),
            dma((2, FIELDS)),
            dma((FIELDS,)),
        ],
        compiler_params=pltpu.CompilerParams(vmem_limit_bytes=67043328),
        name="finish",
    )(fields, coef, equiv)
    return static, member, equiv.reshape(OBS)


def solution(mesh):
    both = ("lat", "lon")
    in_specs = (
        P(None, None, "lat", "lon", None), P(), P(), P(), P(), P(both, None),
        P(both), P(both), P(both), P(None, both), P(both), P(both),
    )
    out_specs = (P("lat", "lon", None), P(None, "lat", "lon", None), P(both))
    return jax.shard_map(
        body, mesh=mesh, in_specs=in_specs, out_specs=out_specs, check_vma=False
    )
```

```python
import jax
import jax.numpy as jnp
from jax import lax
from jax.experimental import pallas as pl
from jax.experimental.pallas import tpu as pltpu
from jax.sharding import PartitionSpec as P

F32 = jnp.float32
BF16 = jnp.bfloat16
MESH = pl.DeviceIdType.MESH
SMOOTH = 0.15
BETA_STATIC = 0.5
BETA_ENSEMBLE = 0.85
NLAT, NLON = 8, 32
MEM, WIN, ROWS, COLS, LEV, NINST = 8, 4, 4, 48, 128, 16
FIELDS = MEM + 1
EARLY = 6
CELLS = ROWS * COLS
OBS = 256
SLOTS = 2 * OBS
PAD = 8
WIDE = COLS + 2 * PAD
TALL = 3 * ROWS
OWN = pl.ds(PAD, COLS)


def dot(a, b, precision=None):
    return lax.dot_general(
        a, b, (((1,), (0,)), ((), ())), precision=precision, preferred_element_type=F32
    )


def dot_t(a, b, precision=None):
    return lax.dot_general(
        a, b, (((1,), (1,)), ((), ())), precision=precision, preferred_element_type=F32
    )


def split(x):
    high = x.astype(BF16)
    return high, (x - high.astype(F32)).astype(BF16)


def dot3(x, w_high, w_low):
    high, low = split(x)
    return dot(high, w_high) + (dot(low, w_high) + dot(high, w_low))


def pick_rows(onehot, x):
    high, low = split(x)
    return dot(onehot, high) + dot(onehot, low)


def iota(shape, dim):
    return lax.broadcasted_iota(jnp.int32, shape, dim)


def total(x):
    return jnp.sum(jnp.sum(x, axis=1, keepdims=True), axis=0, keepdims=True)


def fold(x):
    return jnp.sum(x.reshape(COLS // 8, 8, LEV), axis=0)


def kernel(
    count_ref, ens_hbm, vert_hbm, static_hbm, inst_hbm, err_hbm, dest_hbm,
    patch_hbm, window_hbm, instr_hbm, hweight_hbm, innov_hbm,
    out_fields, out_coef, out_equiv,
    ens, vert_ref, static_ref, inst_ref, err_ref, dest_ref,
    patch_ref, window_ref, instr_ref, hweight_ref, innov_ref,
    err_wide, send1, first1, block1, second1, send2, first2, block2, second2, arrived,
    red_a_send, red_a, red_b_send, red_b,
    level_w, place_f, place_w, place_wt, onehot, onehot_t, spread_w, rinv, obs_e, obs_z,
    grad, incr, reg, strip_send, strip_recv, corner_send, corner_recv, tally, stage_a, stage_b, resid, acc,
    in_sem, ens_sem, out_sem, x1, y1, x2, y2, ra, rb, hs, hr,
):
    lat = lax.axis_index("lat")
    lon = lax.axis_index("lon")
    has_n = lat > 0
    has_s = lat < NLAT - 1
    west = lax.rem(lon + NLON - 1, NLON)
    east = lax.rem(lon + 1, NLON)

    big = lat * 4 + lon // 8
    little = lax.rem(lon, 8)

    def big_peer(j):
        return j // 4, lax.rem(j, 4) * 8 + little

    def little_peer(i):
        return lat, (lon // 8) * 8 + i

    barrier = pltpu.get_barrier_semaphore()

    def greet(i, j):
        pl.semaphore_signal(barrier, inc=1, device_id=(i, j), device_id_type=MESH)

    def greet_big(d, c):
        greet(*big_peer(lax.rem(big + d, NLON)))
        return c

    def greet_little(d, c):
        greet(*little_peer(lax.rem(little + d, NLAT)))
        return c

    small = [
        (dest_hbm, dest_ref), (patch_hbm, patch_ref), (window_hbm, window_ref),
        (instr_hbm, instr_ref), (hweight_hbm, hweight_ref), (innov_hbm, innov_ref),
        (vert_hbm, vert_ref), (static_hbm, static_ref), (inst_hbm, inst_ref),
        (err_hbm, err_ref),
    ]
    loads = [
        pltpu.make_async_copy(a, b, in_sem.at[n]) for n, (a, b) in enumerate(small)
    ]
    for c in loads:
        c.start()
    lax.fori_loop(1, NLON, greet_big, 0)
    lax.fori_loop(1, NLAT, greet_little, 0)
    for step in (0, 1, NLAT - 1):
        greet(lax.rem(lat + step, NLAT), west)
        greet(lax.rem(lat + step, NLAT), east)
    ens_copy = pltpu.make_async_copy(ens_hbm, ens, ens_sem)
    ens_copy.start()
    for c in loads:
        c.wait()

    dest_row = dest_ref[...]
    dest_row = (dest_row & 7) * 32 + (dest_row >> 3)
    square0 = iota((OBS, OBS), 0)
    square1 = iota((OBS, OBS), 1)
    dest_f = jnp.where(square0 == square1, dest_row.astype(F32), 0.0)
    dest_col = jnp.sum(dest_f, axis=1, keepdims=True)
    same = (dest_col == dest_row.astype(F32)) & (square0 < square1)
    rank = jnp.sum(same.astype(F32), axis=0, keepdims=True)
    group = (7 - (dest_row >> 5)) * 2 + rank.astype(jnp.int32)
    active = (iota((1, OBS), 1) < count_ref[0]).astype(F32)
    words = jnp.concatenate(
        [
            patch_ref[...].astype(F32),
            window_ref[...].astype(F32),
            instr_ref[...].astype(F32),
            hweight_ref[...] * active,
            innov_ref[...],
        ],
        axis=0,
    )
    tiled = jnp.concatenate([words] * 16, axis=0)
    tiled = jnp.where((iota((128, OBS), 0) >> 3) == group, tiled, 0.0)
    to_big = (iota((NLON, OBS), 0) == (dest_row & 31)).astype(F32)
    outgoing = dot_t(to_big, tiled, lax.Precision.HIGHEST)
    for j in range(NLON):
        send1[j] = outgoing[j : j + 1, :]

    err_wide[...] = jnp.ones_like(err_wide)
    err_wide[:, 0:NINST] = err_ref[...]
    for n, ref in enumerate((vert_ref, static_ref)):
        w = ref[...]
        level_w[n, 0], level_w[n, 1] = split(w)
        level_w[n, 2], level_w[n, 3] = split(w.T)
    place_f[...] = jnp.zeros_like(place_f)
    for c in range(4):
        place_f[16 * c : 16 * c + 16, LEV * c : LEV * c + LEV] = inst_ref[...]
    for n, half in enumerate(split(place_f[...])):
        place_w[n] = half
    for c in range(4):
        for n, half in enumerate(split(place_f[:, LEV * c : LEV * c + LEV].T)):
            place_wt[n, LEV * c : LEV * c + LEV, :] = half
    for a in range(2):
        reg[a, :, :, 0:PAD, :] = jnp.zeros((FIELDS, TALL, PAD, LEV), F32)
        reg[a, :, :, PAD + COLS : WIDE, :] = jnp.zeros((FIELDS, TALL, PAD, LEV), F32)
    acc[...] = jnp.zeros_like(acc)
    incr[...] = jnp.zeros_like(incr)

    pl.semaphore_wait(barrier, NLON - 1 + NLAT - 1 + 6)

    def remote(src, dst, ssem, rsem, i, j):
        return pltpu.make_async_remote_copy(
            src_ref=src, dst_ref=dst, send_sem=ssem, recv_sem=rsem,
            device_id=(i, j), device_id_type=MESH,
        )

    def rows_done(rows, ssem, rsem):
        ref = tally.at[pl.ds(0, rows)]
        return remote(ref, ref, ssem, rsem, lat, east)

    def rows_to_big(send, first, sems, one_row):
        def go(d, c):
            j = lax.rem(big + d, NLON)
            src = send if one_row else send.at[j]
            remote(src, first.at[big], sems.at[0], sems.at[1], *big_peer(j)).start()
            return c

        lax.fori_loop(1, NLON, go, 0)
        first[big] = send[...] if one_row else send[big]

    def all_big(sems):
        return rows_done(NLON - 1, sems.at[0], sems.at[1])

    def block_to_little(send, second, sems, whole):
        def go(d, c):
            i = lax.rem(little + d, NLAT)
            src = send if whole else send.at[i]
            to = little_peer(i)
            remote(src, second.at[little], sems.at[0], sems.at[1], *to).start()
            return c

        lax.fori_loop(1, NLAT, go, 0)
        second[little] = send[...] if whole else send[little]

    def all_little(sems, rows):
        return rows_done((NLAT - 1) * rows, sems.at[0], sems.at[1])

    lanes8 = iota((8, 128), 1) >> 4

    def exchange(send, first, block, second, xs, ys):
        rows_to_big(send, first, xs, False)
        all_big(xs).wait_recv()
        for q in range(4):
            swapped = jnp.zeros((8, 128), F32)
            for n in range(8):
                row = jnp.broadcast_to(first[8 * q + n], (8, 128))
                row = pltpu.roll(row, 0, 1, stride=16, stride_axis=0)
                if n > 0:
                    row = pltpu.roll(row, 128 - 16 * n, 1)
                swapped = jnp.where(lanes8 == 7 - n, row, swapped)
            for i in range(NLAT):
                block[i, q : q + 1, :] = swapped[i : i + 1, :]
        block_to_little(block, second, ys, False)
        all_little(ys, 4).wait_recv()
        for i in range(NLAT):
            for q in range(4):
                row = jnp.broadcast_to(second[i, q : q + 1, :], (8, 128))
                row = pltpu.roll(row, 16, 1, stride=16, stride_axis=0)
                at = (i * 4 + q) * 8
                arrived[at : at + 8, :] = row
        return arrived[...]

    received = exchange(send1, first1, block1, second1, x1, y1)

    lane = iota((OBS, 128), 1)
    inst_lane = (lane & 15).astype(F32)
    err_row = err_wide[...]
    rinv_row = 1.0 / (err_row * err_row)
    row_w = iota((128, 128), 0)
    col_w = iota((128, 128), 1)
    ids = received.astype(BF16)
    for s in range(2):
        at = 8 * s
        here = slice(s * OBS, (s + 1) * OBS)
        l0 = iota((128, OBS), 0)
        pick = jnp.where(l0 == at, 1.0, 0.0) + jnp.where(l0 == at + 1, 48.0, 0.0)
        l1 = iota((OBS, 128), 1)
        pick_t = jnp.where(l1 == at, 1.0, 0.0) + jnp.where(l1 == at + 1, 48.0, 0.0)
        hot = dot(ids, pick.astype(BF16)) == square1.astype(F32)
        onehot[here, :] = hot.astype(F32).astype(BF16)
        hot_t = dot_t(pick_t.astype(BF16), ids) == square0.astype(F32)
        onehot_t[:, here] = hot_t.astype(F32).astype(BF16)
        instr = dot(ids, jnp.where(row_w == at + 2, 1.0, 0.0).astype(BF16))
        corner = jnp.where((row_w == at + 3 + (col_w >> 4)) & (col_w < 64), 1.0, 0.0)
        hit = instr == inst_lane
        chosen = dot(received, corner, lax.Precision.HIGHEST)
        spread_w[here, :] = jnp.where(hit, chosen, 0.0)
        err_hit = jnp.where(hit & (lane < 16), rinv_row, 0.0)
        inv = jnp.sum(err_hit, axis=1, keepdims=True)
        rinv[here, :] = jnp.broadcast_to(inv, (OBS, 128))
        obs_z[here, :] = jnp.broadcast_to(received[:, at + 7 : at + 8], (OBS, 128))

    ens_copy.wait()

    def gradient(weights):
        table = pick_rows(onehot_t[...], spread_w[...] * (rinv[...] * weights[...]))
        table = table[:CELLS]
        for h in range(2):
            wide = slice(h * 2 * LEV, (h + 1) * 2 * LEV)
            both = dot3(table, place_w[0, :, wide], place_w[1, :, wide])
            for c2 in range(2):
                field = both[:, c2 * LEV : (c2 + 1) * LEV]
                for t in range(WIN):
                    for pr in range(2):
                        at = (t * 2 + pr) * 24
                        grad[t, 2 * pr + h, pl.ds(c2, 24, stride=2), :] = field[
                            at : at + 24
                        ]

    def halo_copies(a, k):
        own = reg.at[a, k, pl.ds(ROWS, ROWS), OWN]
        north_rows = reg.at[a, k, pl.ds(0, ROWS), OWN]
        south_rows = reg.at[a, k, pl.ds(2 * ROWS, ROWS), OWN]
        w_strip = strip_send.at[a, k, 0]
        e_strip = strip_send.at[a, k, 1]

        def one(src, dst, part, i, j):
            return remote(src, dst, hs.at[a, part], hr.at[a, part, k], i, j)

        def corner(n, m):
            return corner_send.at[a, k, n], corner_recv.at[a, k, m]

        always = [
            one(w_strip, strip_recv.at[a, k, 1], 0, lat, west),
            one(e_strip, strip_recv.at[a, k, 0], 0, lat, east),
        ]
        to_n = [
            one(own, south_rows, 2, lat - 1, lon),
            one(*corner(0, 3), 2, lat - 1, west),
            one(*corner(1, 2), 2, lat - 1, east),
        ]
        to_s = [
            one(own, north_rows, 1, lat + 1, lon),
            one(*corner(2, 1), 1, lat + 1, west),
            one(*corner(3, 0), 1, lat + 1, east),
        ]
        return always, to_n, to_s

    def start_halo(a, k):
        always, to_n, to_s = halo_copies(a, k)

        @pl.when(has_n)
        def _():
            for c in to_n:
                c.start()

        @pl.when(has_s)
        def _():
            for c in to_s:
                c.start()

        for c in always:
            c.start()

    def wait_halo(a, k):
        rows_done(32, hs.at[a, 0], hr.at[a, 0, k]).wait_recv()

        @pl.when(has_n)
        def _():
            rows_done(CELLS + 16, hs.at[a, 1], hr.at[a, 1, k]).wait_recv()

        @pl.when(has_s)
        def _():
            rows_done(CELLS + 16, hs.at[a, 2], hr.at[a, 2, k]).wait_recv()

    def sent_halo(a):
        rows_done(FIELDS * 32, hs.at[a, 0], hr.at[a, 0, 0]).wait_send()

        @pl.when(has_s)
        def _():
            rows_done(FIELDS * (CELLS + 16), hs.at[a, 1], hr.at[a, 1, 0]).wait_send()

        @pl.when(has_n)
        def _():
            rows_done(FIELDS * (CELLS + 16), hs.at[a, 2], hr.at[a, 2, 0]).wait_send()

    def put_own(a, k, flat):
        for r in range(ROWS):
            row = flat[r * COLS : (r + 1) * COLS]
            reg[a, k, ROWS + r, PAD : PAD + COLS, :] = row
            strip_send[a, k, 0, 4 * r : 4 * r + 4, :] = row[0:4]
            strip_send[a, k, 1, 4 * r : 4 * r + 4, :] = row[COLS - 4 : COLS]
            for south in range(2):
                near = ROWS - 1 - r if south else r
                if near < 3:
                    at = (0, 3, 5)[near]
                    n = 3 - near
                    corner_send[a, k, 2 * south, at : at + n, :] = row[0:n]
                    corner_send[a, k, 2 * south + 1, at : at + n, :] = row[COLS - n : COLS]

    def send_fields(a):
        def member(k, c):
            summed = ens[k, 0].astype(F32) * grad[0]
            for t in range(1, WIN):
                summed = summed + ens[k, t].astype(F32) * grad[t]
            flat = dot3(summed.reshape(CELLS, LEV), level_w[0, 2], level_w[0, 3])
            put_own(a, k, BETA_ENSEMBLE * flat)
            start_halo(a, k)
            return c

        lax.fori_loop(0, MEM, member, 0)
        summed = (grad[0] + grad[1]) + (grad[2] + grad[3])
        flat = dot3(summed.reshape(CELLS, LEV), level_w[1, 2], level_w[1, 3])
        put_own(a, MEM, BETA_STATIC * flat)
        start_halo(a, MEM)

    def smooth(up, mid, down):
        side = pltpu.roll(mid, 1, 0) + pltpu.roll(mid, WIDE - 1, 0)
        return (1.0 - 4.0 * SMOOTH) * mid + SMOOTH * (up + down + side)

    def keep(row, value):
        if row < ROWS:
            return jnp.where(has_n, value, 0.0)
        if row >= 2 * ROWS:
            return jnp.where(has_s, value, 0.0)
        return value

    def spread_twice(a, k, note):
        for side, col in ((0, PAD - 4), (1, PAD + COLS)):
            for r in range(ROWS):
                reg[a, k, ROWS + r, col : col + 4, :] = strip_recv[
                    a, k, side, 4 * r : 4 * r + 4, :
                ]
            for south in range(2):
                for near in range(3):
                    at = (0, 3, 5)[near]
                    n = 3 - near
                    row = 2 * ROWS + near if south else ROWS - 1 - near
                    first_col = PAD + COLS if side else PAD - n
                    reg[a, k, row, first_col : first_col + n, :] = corner_recv[
                        a, k, 2 * south + side, at : at + n, :
                    ]

        def sweep(read, write, low, high):
            rows = [read(low - 1), read(low)]
            for r in range(low, high):
                rows.append(read(r + 1))
                write(r, keep(r, smooth(rows[0], rows[1], rows[2])))
                rows = rows[1:]

        def to_a(r, v):
            stage_a[r] = v

        def to_b(r, v):
            stage_b[r] = v

        sweep(lambda r: keep(r, reg[a, k, r]), to_a, 1, TALL - 1)
        sweep(lambda r: stage_a[r], to_b, 2, TALL - 2)
        for r in range(ROWS):
            note(k, r, stage_b[ROWS + r, PAD : PAD + COLS, :])
        sweep(lambda r: stage_b[r], to_a, 3, TALL - 3)
        sweep(lambda r: stage_a[r], to_b, 4, TALL - 4)
        rows = [stage_b[ROWS + r, PAD : PAD + COLS, :] for r in range(ROWS)]
        return jnp.concatenate(rows, axis=0)

    def apply_members(a, start, stop, note):
        def member(k, c):
            wait_halo(a, k)
            local = dot3(spread_twice(a, k, note), level_w[0, 0], level_w[0, 1])
            local = (BETA_ENSEMBLE * local).reshape(ROWS, COLS, LEV)
            for t in range(WIN):
                incr[t] += ens[k, t].astype(F32) * local
            return c

        lax.fori_loop(start, stop, member, 0)

    def apply_static(a, target, note):
        wait_halo(a, MEM)
        part = dot3(spread_twice(a, MEM, note), level_w[1, 0], level_w[1, 1])
        part = (BETA_STATIC * part).reshape(ROWS, COLS, LEV)
        for t in range(WIN):
            incr[t] += part
        seen = jnp.zeros((CELLS, 128), F32)
        for h in range(2):
            pair = []
            for c2 in range(2):
                cells = [
                    incr[t, 2 * pr + h, pl.ds(c2, 24, stride=2), :]
                    for t in range(WIN)
                    for pr in range(2)
                ]
                pair.append(jnp.concatenate(cells, axis=0))
            tall = slice(h * 2 * LEV, (h + 1) * 2 * LEV)
            seen = seen + dot3(
                jnp.concatenate(pair, axis=1), place_wt[0, tall, :], place_wt[1, tall, :]
            )
        seen = jnp.concatenate([seen, jnp.zeros((OBS - CELLS, 128), F32)], axis=0)
        value = pick_rows(onehot[...], seen) * spread_w[...]
        value = jnp.sum(value, axis=1, keepdims=True)
        target[...] = jnp.broadcast_to(value, (SLOTS, 128))

    def note_first(k, r, v):
        resid[0, k, r] = v
        acc[0] += fold(v * v)

    gradient(obs_z)
    send_fields(0)
    apply_members(0, 0, MEM, note_first)
    apply_static(0, obs_e, note_first)
    out0 = pltpu.make_async_copy(resid.at[0], out_fields.at[0], out_sem.at[0])
    out0.start()
    sum_a = total(acc[0])
    first_e = obs_e[...]
    sum_b = jnp.sum(rinv[...] * first_e * first_e, axis=0, keepdims=True)[:, 0:1]
    lane1 = iota((1, 128), 1)
    red_a_send[...] = jnp.where(lane1 == 0, sum_a, 0.0) + jnp.where(lane1 == 1, sum_b, 0.0)
    rows_to_big(red_a_send, red_a, ra, True)

    incr[...] = jnp.zeros_like(incr)
    acc[...] = jnp.zeros_like(acc)
    gradient(obs_e)
    send_fields(1)
    def note_early(k, r, v):
        resid[1, k, r] = v

    apply_members(1, 0, 1, note_early)
    all_big(ra).wait_recv()
    part = red_a[0]
    for j in range(1, NLON):
        part = part + red_a[j]
    red_b_send[...] = part
    block_to_little(red_b_send, red_b, rb, True)
    apply_members(1, 1, EARLY, note_early)
    all_little(rb, 1).wait_recv()
    whole = red_b[0]
    for i in range(1, NLAT):
        whole = whole + red_b[i]
    a0 = whole[:, 0:1]
    b0 = whole[:, 1:2]
    step0 = a0 / (a0 + b0)
    rest0 = b0 / (a0 + b0)

    def note_second(k, r, v):
        r0 = resid[0, k, r]
        r1 = rest0 * r0 - step0 * v
        resid[1, k, r] = r1
        acc[0] += fold(r1 * r1)
        acc[1] += fold(r1 * r0)

    def catch_up(k, c):
        for r in range(ROWS):
            note_second(k, r, resid[1, k, r])
        return c

    lax.fori_loop(0, EARLY, catch_up, 0)
    apply_members(1, EARLY, MEM, note_second)
    apply_static(1, obs_z, note_second)
    out1 = pltpu.make_async_copy(resid.at[1], out_fields.at[1], out_sem.at[1])
    out1.start()

    partial = [total(acc[0]), total(acc[1])]
    sum_v = jnp.zeros((1, 1), F32)
    sum_w = jnp.zeros((1, 1), F32)
    blocks = jnp.zeros((OBS, 128), F32)
    word = lane & 15
    for s in range(2):
        here = slice(s * OBS, (s + 1) * OBS)
        e = obs_e[here, :]
        nxt = rest0 * e - step0 * obs_z[here, :]
        weighted = rinv[here, :] * nxt
        sum_v = sum_v + jnp.sum(weighted * nxt, axis=0, keepdims=True)[:, 0:1]
        sum_w = sum_w + jnp.sum(weighted * e, axis=0, keepdims=True)[:, 0:1]
        blocks = jnp.where(word == s, e, blocks)
        blocks = jnp.where(word == 2 + s, nxt, blocks)
    partial = partial + [sum_v, sum_w]
    for n in range(4):
        blocks = jnp.where(word == 4 + n, partial[n], blocks)
    blocks = jnp.where((lane >> 4) == 7 - (iota((OBS, 128), 0) >> 5), blocks, 0.0)
    out_rows = blocks[0:NLON]
    for i in range(1, NLAT):
        out_rows = out_rows + blocks[i * NLON : (i + 1) * NLON]
    for j in range(NLON):
        send2[j] = out_rows[j : j + 1, :]

    back = exchange(send2, first2, block2, second2, x2, y2)
    sums = jnp.sum(back, axis=0, keepdims=True)
    rr1, u, v, w = [sums[:, 4 + n : 5 + n] for n in range(4)]
    ratio = rr1 / a0
    below = (rr1 + 2.0 * ratio * u + ratio * ratio * a0) + (
        v + 2.0 * ratio * w + ratio * ratio * b0
    )
    step1 = rr1 / below
    c0 = step0 + step1 * ratio
    c1 = step1
    out_coef[...] = jnp.where(iota((2, 128), 0) == 0, c0, c1)

    mine = dest_row == square0
    equiv = jnp.zeros((1, OBS), F32)
    for s in range(2):
        value = c0 * back[:, s : s + 1] + c1 * back[:, 2 + s : 3 + s]
        chosen = jnp.where(mine & (rank == float(s)), value, 0.0)
        equiv = equiv + jnp.sum(chosen, axis=0, keepdims=True)
    out_equiv[...] = equiv

    out0.wait()
    out1.wait()
    for sems in (x1, x2, ra):
        all_big(sems).wait_send()
    for sems, rows in ((y1, 4), (y2, 4), (rb, 1)):
        all_little(sems, rows).wait_send()
    sent_halo(0)
    sent_halo(1)


def finish(fields, coef, equiv, out_static, out_member, out_equiv, held, made, sem_in, sem_out):
    loads = [
        [pltpu.make_async_copy(fields.at[a, k], held.at[a, k], sem_in.at[a, k]) for a in range(2)]
        for k in range(FIELDS)
    ]
    for pair in loads:
        for c in pair:
            c.start()
    out_equiv[...] = equiv[...]
    c0 = coef[0:1, :]
    c1 = coef[1:2, :]
    stores = []
    for k in range(FIELDS):
        for c in loads[k]:
            c.wait()
        for r in range(ROWS):
            made[k, r] = c0 * held[0, k, r] + c1 * held[1, k, r]
        target = out_static if k == MEM else out_member.at[k]
        stores.append(pltpu.make_async_copy(made.at[k], target, sem_out.at[k]))
        stores[-1].start()
    for c in stores:
        c.wait()


def body(
    ensemble, vert_loc, static_vert, inst_vert, inst_err, obs_dest, obs_patch,
    obs_window, obs_inst, obs_hweight, innovation, obs_count,
):
    vmem = pl.BlockSpec(memory_space=pltpu.VMEM)
    anywhere = pl.BlockSpec(memory_space=pl.ANY)
    hbm = pl.BlockSpec(memory_space=pltpu.HBM)
    dma = pltpu.SemaphoreType.DMA
    ints = jnp.int32
    exchange = [
        pltpu.VMEM((NLON, 1, 128), F32),
        pltpu.VMEM((NLON, 1, 128), F32),
        pltpu.VMEM((NLAT, 4, 128), F32),
        pltpu.VMEM((NLAT, 4, 128), F32),
    ]
    scratch = [
        pltpu.VMEM((MEM, WIN, ROWS, COLS, LEV), BF16),
        pltpu.VMEM((LEV, LEV), F32),
        pltpu.VMEM((LEV, LEV), F32),
        pltpu.VMEM((NINST, LEV), F32),
        pltpu.VMEM((1, NINST), F32),
        pltpu.VMEM((1, OBS), ints),
        pltpu.VMEM((1, OBS), ints),
        pltpu.VMEM((1, OBS), ints),
        pltpu.VMEM((1, OBS), ints),
        pltpu.VMEM((4, OBS), F32),
        pltpu.VMEM((1, OBS), F32),
        pltpu.VMEM((1, 128), F32),
        *exchange,
        *exchange,
        pltpu.VMEM((OBS, 128), F32),
        pltpu.VMEM((1, 128), F32),
        pltpu.VMEM((NLON, 1, 128), F32),
        pltpu.VMEM((1, 128), F32),
        pltpu.VMEM((NLAT, 1, 128), F32),
        pltpu.VMEM((2, 4, LEV, LEV), BF16),
        pltpu.VMEM((128, 4 * LEV), F32),
        pltpu.VMEM((2, 128, 4 * LEV), BF16),
        pltpu.VMEM((2, 4 * LEV, 128), BF16),
        pltpu.VMEM((SLOTS, OBS), BF16),
        pltpu.VMEM((OBS, SLOTS), BF16),
        pltpu.VMEM((SLOTS, 128), F32),
        pltpu.VMEM((SLOTS, 128), F32),
        pltpu.VMEM((SLOTS, 128), F32),
        pltpu.VMEM((SLOTS, 128), F32),
        pltpu.VMEM((WIN, ROWS, COLS, LEV), F32),
        pltpu.VMEM((WIN, ROWS, COLS, LEV), F32),
        pltpu.VMEM((2, FIELDS, TALL, WIDE, LEV), F32),
        pltpu.VMEM((2, FIELDS, 2, 16, LEV), F32),
        pltpu.VMEM((2, FIELDS, 2, 16, LEV), F32),
        pltpu.VMEM((2, FIELDS, 4, 8, LEV), F32),
        pltpu.VMEM((2, FIELDS, 4, 8, LEV), F32),
        pltpu.VMEM((FIELDS * (CELLS + 16), 128), F32),
        pltpu.VMEM((TALL, WIDE, LEV), F32),
        pltpu.VMEM((TALL, WIDE, LEV), F32),
        pltpu.VMEM((2, FIELDS, ROWS, COLS, LEV), F32),
        pltpu.VMEM((2, 8, LEV), F32),
        dma((10,)), dma(()), dma((2,)),
        dma((2,)), dma((2,)), dma((2,)), dma((2,)), dma((2,)), dma((2,)),
        dma((2, 3)), dma((2, 3, FIELDS)),
    ]
    fields, coef, equiv = pl.pallas_call(
        kernel,
        out_shape=(
            jax.ShapeDtypeStruct((2, FIELDS, ROWS, COLS, LEV), F32),
            jax.ShapeDtypeStruct((2, 128), F32),
            jax.ShapeDtypeStruct((1, OBS), F32),
        ),
        in_specs=[pl.BlockSpec(memory_space=pltpu.SMEM)] + [hbm] * 11,
        out_specs=(anywhere, vmem, vmem),
        scratch_shapes=scratch,
        compiler_params=pltpu.CompilerParams(
            collective_id=0, has_side_effects=True, vmem_limit_bytes=67043328
        ),
        name="inner_loop",
    )(
        obs_count, ensemble, vert_loc, static_vert, inst_vert,
        inst_err.reshape(1, NINST), obs_dest.reshape(1, OBS),
        obs_patch.reshape(1, OBS), obs_window.reshape(1, OBS),
        obs_inst.reshape(1, OBS), obs_hweight, innovation.reshape(1, OBS),
    )
    static, member, equiv = pl.pallas_call(
        finish,
        out_shape=(
            jax.ShapeDtypeStruct((ROWS, COLS, LEV), F32),
            jax.ShapeDtypeStruct((MEM, ROWS, COLS, LEV), F32),
            jax.ShapeDtypeStruct((1, OBS), F32),
        ),
        in_specs=[hbm, vmem, vmem],
        out_specs=(hbm, hbm, vmem),
        scratch_shapes=[
            pltpu.VMEM((2, FIELDS, ROWS, COLS, LEV), F32),
            pltpu.VMEM((FIELDS, ROWS, COLS, LEV), F32),
            dma((2, FIELDS)),
            dma((FIELDS,)),
        ],
        compiler_params=pltpu.CompilerParams(vmem_limit_bytes=67043328),
        name="finish",
    )(fields, coef, equiv)
    return static, member, equiv.reshape(OBS)


def solution(mesh):
    both = ("lat", "lon")
    in_specs = (
        P(None, None, "lat", "lon", None), P(), P(), P(), P(), P(both, None),
        P(both), P(both), P(both), P(None, both), P(both), P(both),
    )
    out_specs = (P("lat", "lon", None), P(None, "lat", "lon", None), P(both))
    return jax.shard_map(
        body, mesh=mesh, in_specs=in_specs, out_specs=out_specs, check_vma=False
    )
```
